8 devices in a mesh: tp: 2 (over z, y), cp: 4 (over x, core).
Axes of the slice: x: 2, y: 2, z: 1, core: 2. Of those that a mesh axis runs over, the one named last changes fastest.
Arguments:
- x_rows: bfloat16 [4096, 3072], P(('cp', 'tp'))
- grad_y: bfloat16 [4096, 3072], P(('cp', 'tp'))
- positions: int32 [4096], P('cp')
- gamma_attn: bfloat16 [3072], replicated
- gamma_mlp: bfloat16 [3072], replicated
- w_q: bfloat16 [3072, 3072], P(None, 'tp')
- w_k: bfloat16 [3072, 1024], P(None, 'tp')
- w_v: bfloat16 [3072, 1024], P(None, 'tp')
- w_out: bfloat16 [3072, 3072], P('tp')
- w_gate: bfloat16 [3072, 8192], P(None, 'tp')
- w_up: bfloat16 [3072, 8192], P(None, 'tp')
- w_down: bfloat16 [8192, 3072], P('tp')
Outputs:
- output 1: bfloat16 [4096, 3072], P(('cp', 'tp'))
- output 2: bfloat16 [4096, 3072], P(('cp', 'tp'))
- output 3: float32 [3072], replicated
- output 4: float32 [3072], replicated
- output 5: float32 [3072, 3072], P(None, 'tp')
- output 6: float32 [3072, 1024], P(None, 'tp')
- output 7: float32 [3072, 1024], P(None, 'tp')
- output 8: float32 [3072, 3072], P('tp')
- output 9: float32 [3072, 8192], P(None, 'tp')
- output 10: float32 [3072, 8192], P(None, 'tp')
- output 11: float32 [8192, 3072], P('tp')
All inputs are finite; a program needn't handle non-finite values.
Results may differ from the reference program's by a relative error of at most 0.02.
Values are sent between devices in bfloat16 or wider.
A program may use at most 1.25 GiB of HBM per device.

```python
import functools
import jax
import jax.numpy as jnp
from jax import lax

D = 3072
HEADS = 24
KV_HEADS = 8
HEAD = 128
FF = 8192
SEQ = 4096
CP_RANKS = 4
QUERY_BLOCK = 128
GROUPS = HEADS // KV_HEADS
EPS = 1e-5
ROPE_BASE = 500000.0


def matmul32(left, right):
    return jnp.dot(left.astype(jnp.float32), right.astype(jnp.float32))


def rms_norm(rows, gamma):
    rows_f = rows.astype(jnp.float32)
    inv_rms = lax.rsqrt(jnp.mean(rows_f * rows_f, axis=-1, keepdims=True) + EPS)
    return (rows_f * inv_rms * gamma.astype(jnp.float32)).astype(jnp.bfloat16)


def rope_tables(positions):
    inv_freq = ROPE_BASE ** (-jnp.arange(0, HEAD, 2, dtype=jnp.float32) / HEAD)
    angles = positions.astype(jnp.float32)[:, None] * inv_freq[None, :]
    return jnp.cos(angles)[:, None, :], jnp.sin(angles)[:, None, :]


def rotate(heads_in, cosine, sine):
    half = HEAD // 2
    first = heads_in[..., :half]
    second = heads_in[..., half:]
    return jnp.concatenate([first * cosine - second * sine, second * cosine + first * sine], axis=-1)


def attention(queries, keys, values, positions):
    keys_f = keys.astype(jnp.float32)
    values_f = values.astype(jnp.float32)
    count = SEQ // QUERY_BLOCK

    def one_block(block_args):
        q_block, q_pos = block_args
        scores = jnp.einsum('qkgd,tkd->qkgt', q_block.astype(jnp.float32), keys_f) * HEAD ** -0.5
        visible = (positions[None, :] <= q_pos[:, None])[:, None, None, :]
        probs = jax.nn.softmax(jnp.where(visible, scores, -1e30), axis=-1)
        return jnp.einsum('qkgt,tkd->qkgd', probs, values_f)

    blocks = lax.map(jax.checkpoint(one_block), (queries.reshape(count, QUERY_BLOCK, KV_HEADS, GROUPS, HEAD), positions.reshape(count, QUERY_BLOCK)))
    return blocks.reshape(SEQ, HEADS * HEAD)


def layer(x_rows, gamma_attn, gamma_mlp, w_q, w_k, w_v, w_out, w_gate, w_up, w_down, positions):
    cosine, sine = rope_tables(positions)
    h_attn = rms_norm(x_rows, gamma_attn)
    queries = rotate(matmul32(h_attn, w_q).reshape(SEQ, HEADS, HEAD), cosine, sine).astype(jnp.bfloat16)
    keys = rotate(matmul32(h_attn, w_k).reshape(SEQ, KV_HEADS, HEAD), cosine, sine).astype(jnp.bfloat16)
    values = matmul32(h_attn, w_v).astype(jnp.bfloat16).reshape(SEQ, KV_HEADS, HEAD)
    attn_out = attention(queries.reshape(SEQ, KV_HEADS, GROUPS, HEAD), keys, values, positions).astype(jnp.bfloat16)
    attn_rows = matmul32(attn_out, w_out).astype(jnp.bfloat16)
    mid_rows = (x_rows.astype(jnp.float32) + attn_rows.astype(jnp.float32)).astype(jnp.bfloat16)
    h_mlp = rms_norm(mid_rows, gamma_mlp)
    gate = matmul32(h_mlp, w_gate)
    mlp_hidden = (jax.nn.silu(gate) * matmul32(h_mlp, w_up)).astype(jnp.bfloat16)
    down_rows = matmul32(mlp_hidden, w_down).astype(jnp.bfloat16)
    return (mid_rows.astype(jnp.float32) + down_rows.astype(jnp.float32)).astype(jnp.bfloat16)


def setup_inputs(seed: int = 0) -> dict:
    rand_keys = jax.random.split(jax.random.key(seed), 13)

    def normal(key, shape, scale):
        return (jax.random.normal(key, shape, jnp.float32) * scale).astype(jnp.bfloat16)

    def gain(key):
        return (1.0 + 0.2 * jax.random.normal(key, (D,), jnp.float32)).astype(jnp.bfloat16)

    piece = SEQ // (2 * CP_RANKS)
    gaps = jax.random.randint(rand_keys[12], (SEQ,), 1, 3)
    ordered = jnp.cumsum(gaps) - gaps[0]
    ranks = jnp.arange(CP_RANKS)
    order = jnp.stack([ranks, 2 * CP_RANKS - 1 - ranks], axis=1).reshape(-1)
    positions = ordered.reshape(2 * CP_RANKS, piece)[order].reshape(SEQ).astype(jnp.int32)
    q_cols = HEADS * HEAD
    kv_cols = KV_HEADS * HEAD
    return dict(
        x_rows=normal(rand_keys[0], (SEQ, D), 1.0),
        grad_y=normal(rand_keys[1], (SEQ, D), 1.0),
        positions=positions,
        gamma_attn=gain(rand_keys[2]),
        gamma_mlp=gain(rand_keys[3]),
        w_q=normal(rand_keys[4], (D, q_cols), D ** -0.5),
        w_k=normal(rand_keys[5], (D, kv_cols), D ** -0.5),
        w_v=normal(rand_keys[6], (D, kv_cols), D ** -0.5),
        w_out=normal(rand_keys[7], (q_cols, D), q_cols ** -0.5),
        w_gate=normal(rand_keys[8], (D, FF), D ** -0.5),
        w_up=normal(rand_keys[9], (D, FF), D ** -0.5),
        w_down=normal(rand_keys[10], (FF, D), FF ** -0.5),
    )


def reference(x_rows, grad_y, positions, gamma_attn, gamma_mlp, w_q, w_k, w_v, w_out, w_gate, w_up, w_down):
    primals = [t.astype(jnp.float32) for t in (x_rows, gamma_attn, gamma_mlp, w_q, w_k, w_v, w_out, w_gate, w_up, w_down)]
    y_rows, pullback = jax.vjp(functools.partial(layer, positions=positions), *primals)
    grads = pullback(grad_y)
    return (y_rows, grads[0].astype(jnp.bfloat16), grads[1], grads[2], grads[3], grads[4], grads[5], grads[6], grads[7], grads[8], grads[9])
```

```python
import jax
import jax.numpy as jnp
from jax import lax
from jax.sharding import Mesh, PartitionSpec as P


HEAD_DIM = 128
EPS = 1e-5
ROPE_BASE = 500000.0
NEG_BIG = -1e30
CONTRACT_COLS = (((1,), (1,)), ((), ()))
CONTRACT_ROWS = (((0,), (0,)), ((), ()))


def rms_forward(rows, gamma):
    rows_f = rows.astype(jnp.float32)
    inv_rms = lax.rsqrt(jnp.mean(rows_f * rows_f, axis=-1, keepdims=True) + EPS)
    normed = rows_f * inv_rms
    return (normed * gamma.astype(jnp.float32)).astype(jnp.bfloat16), normed, inv_rms


def rms_backward(grad_out, normed, inv_rms, gamma):
    grad_norm = grad_out * gamma.astype(jnp.float32)
    grad_rows = inv_rms * (grad_norm - normed * jnp.mean(grad_norm * normed, axis=-1, keepdims=True))
    return grad_rows, jnp.sum(grad_out * normed, axis=0)


def rope_tables(positions):
    inv_freq = ROPE_BASE ** (-jnp.arange(0, HEAD_DIM, 2, dtype=jnp.float32) / HEAD_DIM)
    angles = positions.astype(jnp.float32)[:, None] * inv_freq[None, :]
    return jnp.cos(angles)[:, None, :], jnp.sin(angles)[:, None, :]


def rotate(heads_in, cosine, sine):
    half = HEAD_DIM // 2
    first, second = heads_in[..., :half], heads_in[..., half:]
    return jnp.concatenate([first * cosine - second * sine, second * cosine + first * sine], axis=-1)


def rotate_back(grads, cosine, sine):
    half = HEAD_DIM // 2
    first, second = grads[..., :half], grads[..., half:]
    return jnp.concatenate([first * cosine + second * sine, second * cosine - first * sine], axis=-1)


def scores_of(queries, key_block):
    return jnp.einsum('krd,ktd->krt', queries, key_block, preferred_element_type=jnp.float32) * HEAD_DIM ** -0.5


def part_forward(scores, value_block, row_max):
    probs = jnp.exp(scores - row_max[..., None])
    return jnp.sum(probs, axis=-1), jnp.einsum('krt,ktd->krd', probs.astype(jnp.bfloat16), value_block, preferred_element_type=jnp.float32)


def part_backward(queries, key_block, value_block, grad_out, log_sum, delta, visible=None):
    scores = scores_of(queries, key_block)
    if visible is not None:
        scores = jnp.where(visible, scores, NEG_BIG)
    probs = jnp.exp(scores - log_sum[..., None])
    grad_v = jnp.einsum('krt,krd->ktd', probs.astype(jnp.bfloat16), grad_out, preferred_element_type=jnp.float32)
    grad_probs = jnp.einsum('krd,ktd->krt', grad_out, value_block, preferred_element_type=jnp.float32)
    grad_scores = (probs * (grad_probs - delta[..., None]) * HEAD_DIM ** -0.5).astype(jnp.bfloat16)
    grad_q = jnp.einsum('krt,ktd->krd', grad_scores, key_block, preferred_element_type=jnp.float32)
    grad_k = jnp.einsum('krt,krd->ktd', grad_scores, queries, preferred_element_type=jnp.float32)
    return grad_q, grad_k, grad_v


def solution(mesh):
    cp_size = mesh.shape['cp']
    split = Mesh(mesh.devices.reshape(mesh.shape['tp'], cp_size // 2, 2), ('tp', 'cx', 'cc'))
    cp = ('cx', 'cc')
    row_spec = P(('cx', 'cc', 'tp'), None)
    col_spec = P(None, 'tp')
    inner_spec = P('tp', None)
    in_specs = (row_spec, row_spec, P(cp), P(), P(), col_spec, col_spec, col_spec, inner_spec, col_spec, col_spec, inner_spec)
    out_specs = (row_spec, row_spec, P(), P(), col_spec, col_spec, col_spec, inner_spec, col_spec, col_spec, inner_spec)
    swap = [(0, 1), (1, 0)]

    def local(x_rows, grad_y, positions, gamma_attn, gamma_mlp, w_q, w_k, w_v, w_out, w_gate, w_up, w_down):
        span = positions.shape[0]
        half = span // 2
        q_cols = w_q.shape[1]
        kv_cols = w_k.shape[1]
        kv_loc = kv_cols // HEAD_DIM
        groups = q_cols // kv_cols
        rank = lax.axis_index(cp)
        cosine, sine = [t.reshape(2, 1, 1, half, HEAD_DIM // 2) for t in rope_tables(positions)]

        def on_chip(rows):
            return lax.all_gather(rows, 'cc', axis=0, tiled=True)

        def cross(rows):
            return lax.ppermute(rows, 'cx', swap)

        def spread(rows):
            return on_chip(rows), on_chip(cross(rows))

        def spread_shared(rows_own, rows_all):
            other = lax.all_gather(cross(rows_own), 'tp', axis=0, tiled=True)
            return on_chip(rows_all), on_chip(other)

        def weight_grad(left, right):
            return lax.dot_general(left[0], right[0], CONTRACT_ROWS, preferred_element_type=jnp.float32) + lax.dot_general(left[1], right[1], CONTRACT_ROWS, preferred_element_type=jnp.float32)

        def by_head(rows):
            count = rows.shape[1] // HEAD_DIM
            cut = [rows[i * half:(i + 1) * half, n * HEAD_DIM:(n + 1) * HEAD_DIM] for i in range(2) for n in range(count)]
            return jnp.stack(cut).reshape(2, kv_loc, count // kv_loc, half, HEAD_DIM)

        def fold(heads):
            return heads.reshape(2, kv_loc, -1, HEAD_DIM)

        def by_row(early, late):
            return jnp.concatenate([jnp.concatenate([piece[n, m] for n in range(kv_loc) for m in range(piece.shape[1])], axis=1) for piece in (early, late)], axis=0)

        def unfold(piece):
            return piece.reshape(kv_loc, -1, half, HEAD_DIM)

        h_attn, normed_attn, inv_attn = rms_forward(x_rows, gamma_attn)
        h_attn_all = lax.all_gather(h_attn, 'tp', axis=0, tiled=True)
        keys_own = rotate(by_head(jnp.dot(h_attn_all, w_k, preferred_element_type=jnp.float32)), cosine, sine).astype(jnp.bfloat16)
        values_own = by_head(jnp.dot(h_attn_all, w_v, preferred_element_type=jnp.float32).astype(jnp.bfloat16))
        keys_all = lax.all_gather(fold(keys_own), cp, axis=0)
        values_all = lax.all_gather(fold(values_own), cp, axis=0)
        q_heads = by_head(jnp.dot(h_attn_all, w_q, preferred_element_type=jnp.float32))
        queries = fold(rotate(q_heads, cosine, sine).astype(jnp.bfloat16))
        q_early, q_late = queries[0], queries[1]

        def turn(per_rank, start):
            return lax.dynamic_slice_in_dim(jnp.concatenate([per_rank, per_rank], axis=0), start, cp_size, axis=0)

        keys_rel = turn(keys_all, rank)
        values_rel = turn(values_all, rank)

        def join(pieces):
            return pieces.transpose(1, 0, 2, 3).reshape(kv_loc, cp_size * half, HEAD_DIM)

        k_front, v_front = join(keys_rel[:, 0]), join(values_rel[:, 0])
        row_id = lax.broadcasted_iota(jnp.int32, (groups, half, half), 1).reshape(groups * half, half)
        col_id = lax.broadcasted_iota(jnp.int32, (groups * half, half), 1)
        visible = (col_id <= row_id)[None]
        wraps = [rank + d >= cp_size for d in range(1, cp_size)]
        k_pair = [jnp.where(w, keys_rel[d, 0], keys_rel[d, 1]) for d, w in enumerate(wraps, 1)]
        v_pair = [jnp.where(w, values_rel[d, 0], values_rel[d, 1]) for d, w in enumerate(wraps, 1)]
        q_pair = [jnp.where(w, q_early, q_late) for w in wraps]

        s_early = jnp.where(visible, scores_of(q_early, keys_rel[0, 0]), NEG_BIG)
        s_late = jnp.where(visible, scores_of(q_late, keys_rel[0, 1]), NEG_BIG)
        s_front = scores_of(q_late, k_front)
        s_pair = [scores_of(q, k) for q, k in zip(q_pair, k_pair)]
        max_early = jnp.max(s_early, axis=-1)
        max_late = jnp.maximum(jnp.max(s_late, axis=-1), jnp.max(s_front, axis=-1))
        for s, w in zip(s_pair, wraps):
            top = jnp.max(s, axis=-1)
            max_early = jnp.maximum(max_early, jnp.where(w, top, NEG_BIG))
            max_late = jnp.maximum(max_late, jnp.where(w, NEG_BIG, top))
        sum_early, acc_early = part_forward(s_early, values_rel[0, 0], max_early)
        sum_late, acc_late = part_forward(s_late, values_rel[0, 1], max_late)
        sum_front, acc_front = part_forward(s_front, v_front, max_late)
        sum_late, acc_late = sum_late + sum_front, acc_late + acc_front
        for s, v, w in zip(s_pair, v_pair, wraps):
            total, acc = part_forward(s, v, jnp.where(w, max_early, max_late))
            sum_early = sum_early + jnp.where(w, total, 0.0)
            sum_late = sum_late + jnp.where(w, 0.0, total)
            acc_early = acc_early + jnp.where(w, acc, 0.0)
            acc_late = acc_late + jnp.where(w, 0.0, acc)
        out_early = (acc_early / sum_early[..., None]).astype(jnp.bfloat16)
        out_late = (acc_late / sum_late[..., None]).astype(jnp.bfloat16)
        log_early = max_early + jnp.log(sum_early)
        log_late = max_late + jnp.log(sum_late)
        attn_flat = by_row(unfold(out_early), unfold(out_late))
        attn_part = jnp.dot(attn_flat, w_out, preferred_element_type=jnp.float32)
        attn_rows = lax.psum_scatter(attn_part, 'tp', scatter_dimension=0, tiled=True).astype(jnp.bfloat16)
        mid_rows = (x_rows.astype(jnp.float32) + attn_rows.astype(jnp.float32)).astype(jnp.bfloat16)
        h_mlp, normed_mlp, inv_mlp = rms_forward(mid_rows, gamma_mlp)
        h_mlp_all = lax.all_gather(h_mlp, 'tp', axis=0, tiled=True)
        gate = jnp.dot(h_mlp_all, w_gate, preferred_element_type=jnp.float32)
        up_proj = jnp.dot(h_mlp_all, w_up, preferred_element_type=jnp.float32)
        sig_gate = jax.nn.sigmoid(gate)
        silu_gate = gate * sig_gate
        mlp_hidden = (silu_gate * up_proj).astype(jnp.bfloat16)
        down_rows = lax.psum_scatter(jnp.dot(mlp_hidden, w_down, preferred_element_type=jnp.float32), 'tp', scatter_dimension=0, tiled=True).astype(jnp.bfloat16)

        grad_y_all = lax.all_gather(grad_y, 'tp', axis=0, tiled=True)
        grad_hidden = lax.dot_general(grad_y_all, w_down, CONTRACT_COLS, preferred_element_type=jnp.float32)
        grad_gate = (grad_hidden * up_proj * sig_gate * (1.0 + gate * (1.0 - sig_gate))).astype(jnp.bfloat16)
        grad_up = (grad_hidden * silu_gate).astype(jnp.bfloat16)
        grad_h_part = lax.dot_general(grad_gate, w_gate, CONTRACT_COLS, preferred_element_type=jnp.float32)
        grad_h_part = grad_h_part + lax.dot_general(grad_up, w_up, CONTRACT_COLS, preferred_element_type=jnp.float32)
        grad_h_mlp = lax.psum_scatter(grad_h_part, 'tp', scatter_dimension=0, tiled=True)
        grad_mid_norm, grad_gamma_mlp = rms_backward(grad_h_mlp, normed_mlp, inv_mlp, gamma_mlp)
        grad_mid = grad_y.astype(jnp.float32) + grad_mid_norm
        grad_mid_all = lax.all_gather(grad_mid.astype(jnp.bfloat16), 'tp', axis=0, tiled=True)
        grad_attn = fold(by_head(lax.dot_general(grad_mid_all, w_out, CONTRACT_COLS, preferred_element_type=jnp.float32).astype(jnp.bfloat16)))
        g_early, g_late = grad_attn[0], grad_attn[1]
        delta_early = jnp.sum(g_early.astype(jnp.float32) * out_early.astype(jnp.float32), axis=-1)
        delta_late = jnp.sum(g_late.astype(jnp.float32) * out_late.astype(jnp.float32), axis=-1)

        gq_early, gk_e, gv_e = part_backward(q_early, keys_rel[0, 0], values_rel[0, 0], g_early, log_early, delta_early, visible)
        gq_late, gk_l, gv_l = part_backward(q_late, keys_rel[0, 1], values_rel[0, 1], g_late, log_late, delta_late, visible)
        gq_front, gk_front, gv_front = part_backward(q_late, k_front, v_front, g_late, log_late, delta_late)
        gq_front, down_rows = lax.optimization_barrier((gq_front, down_rows))
        gq_late = gq_late + gq_front
        front_k = gk_front.reshape(kv_loc, cp_size, half, HEAD_DIM)
        front_v = gv_front.reshape(kv_loc, cp_size, half, HEAD_DIM)
        gk_rel = [jnp.stack([front_k[:, 0] + gk_e, gk_l])]
        gv_rel = [jnp.stack([front_v[:, 0] + gv_e, gv_l])]
        for d, w in enumerate(wraps, 1):
            gq, gk, gv = part_backward(q_pair[d - 1], k_pair[d - 1], v_pair[d - 1], jnp.where(w, g_early, g_late), jnp.where(w, log_early, log_late), jnp.where(w, delta_early, delta_late))
            gq_early = gq_early + jnp.where(w, gq, 0.0)
            gq_late = gq_late + jnp.where(w, 0.0, gq)
            gk_rel.append(jnp.stack([front_k[:, d] + jnp.where(w, gk, 0.0), jnp.where(w, 0.0, gk)]))
            gv_rel.append(jnp.stack([front_v[:, d] + jnp.where(w, gv, 0.0), jnp.where(w, 0.0, gv)]))
        back = lax.rem(cp_size - rank, cp_size)
        both_rel = jnp.stack([jnp.stack([gk, gv]) for gk, gv in zip(gk_rel, gv_rel)])
        both_own = lax.psum_scatter(turn(both_rel, back).reshape(-1, HEAD_DIM), cp, scatter_dimension=0, tiled=True)
        grad_keys, grad_values = both_own.reshape(2, 2, kv_loc, half, HEAD_DIM)
        grad_q_pre = by_row(*rotate_back(jnp.stack([unfold(gq_early), unfold(gq_late)]), cosine, sine).astype(jnp.bfloat16))
        grad_k_pre = by_row(*rotate_back(jnp.stack([unfold(grad_keys[0]), unfold(grad_keys[1])]), cosine, sine).astype(jnp.bfloat16))
        grad_v_pre = by_row(unfold(grad_values[0]), unfold(grad_values[1])).astype(jnp.bfloat16)
        grad_h_attn = lax.psum_scatter(lax.dot_general(grad_q_pre, w_q, CONTRACT_COLS, preferred_element_type=jnp.float32) + lax.dot_general(grad_k_pre, w_k, CONTRACT_COLS, preferred_element_type=jnp.float32) + lax.dot_general(grad_v_pre, w_v, CONTRACT_COLS, preferred_element_type=jnp.float32), 'tp', scatter_dimension=0, tiled=True)
        grad_x_norm, grad_gamma_attn = rms_backward(grad_h_attn, normed_attn, inv_attn, gamma_attn)
        grad_x = (grad_mid + grad_x_norm).astype(jnp.bfloat16)

        y_rows = (mid_rows.astype(jnp.float32) + down_rows.astype(jnp.float32)).astype(jnp.bfloat16)
        h_attn_parts = spread_shared(h_attn, h_attn_all)
        grad_y_parts = spread_shared(grad_y, grad_y_all)
        attn_parts = spread(attn_flat)
        h_mlp_parts = spread(h_mlp_all)
        grad_w_down = weight_grad(spread(mlp_hidden), grad_y_parts)
        grad_w_gate = weight_grad(h_mlp_parts, spread(grad_gate))
        grad_w_up = weight_grad(h_mlp_parts, spread(grad_up))
        grad_w_out = weight_grad(attn_parts, spread(grad_mid_all))
        grad_w_q = weight_grad(h_attn_parts, spread(grad_q_pre))
        grad_w_k = weight_grad(h_attn_parts, spread(grad_k_pre))
        grad_w_v = weight_grad(h_attn_parts, spread(grad_v_pre))
        gamma_grads = lax.psum((grad_gamma_attn, grad_gamma_mlp), ('tp', 'cx', 'cc'))
        return (y_rows, grad_x) + tuple(gamma_grads) + (grad_w_q, grad_w_k, grad_w_v, grad_w_out, grad_w_gate, grad_w_up, grad_w_down)

    return jax.shard_map(local, mesh=split, in_specs=in_specs, out_specs=out_specs, check_vma=False)
```
